32 devices in a mesh: vert: 8 (over z, x), af: 4 (over y, core).
Axes of the slice: x: 2, y: 2, z: 4, core: 2. Of those that a mesh axis runs over, the one named last changes fastest.
Arguments:
- features_t: bfloat16 [128, 4096], P('af', 'vert'), may hold values from -24 to 24
- weight: bfloat16 [128, 256], P('af'), may hold values from -1 to 1
- bias: float32 [256], P('af'), may hold values from -3 to 3
- self_mask: int32 [8, 512, 512], P('vert'), may hold values 0 or 1
- halo_mask: int32 [8, 6, 512, 256], P('vert'), may hold values 0 or 1
- block_src: int32 [8, 6], P('vert'), may hold values from -1 to 7, as said below
- halo_rows: int32 [8, 6, 256], P('vert'), may hold values from 0 to 511, as said below
- outside_degree: int32 [4096], P('vert'), may hold values from 0 to 47
Outputs:
- output_t: bfloat16 [256, 4096], P('af', 'vert')
The draws below stay inside these ranges and needn't reach their ends.
Inputs may be any that keep to these rules, and one draw needn't show every extreme that they name: `block_src`: the live sources of a row are distinct partitions other than the row's own; empty slots (-1) come after the live ones; every row has at least one live slot and some row has all 6. `halo_rows`: the entries of one slot are distinct.
All inputs are finite; a program needn't handle non-finite values. No bound on the sum of `self_mask` or of `halo_mask` on one device may be relied on, other than what follows from the above.
Results may differ from the reference program's by a relative error of at most 0.0054.
Values may be sent and summed in bfloat16 or wider, within the bound.
A program may use at most 64 MiB of HBM per device.

```python
import jax
import jax.numpy as jnp
from jax import lax

F_IN = 128
F_OUT = 256
BLOCK = 512
NB = 6
HALO = 256
VERTICES = 4096
N_VERT = 8


def shuffled_offsets(one_key):
    return jax.random.permutation(one_key, N_VERT - 1)[:NB]


def shuffled_rows(one_key):
    return jax.random.permutation(one_key, BLOCK)[:HALO]


def draw_block_src(key, part):
    keys = jax.random.split(jax.random.fold_in(key, 11), N_VERT)
    offsets = jax.vmap(shuffled_offsets)(keys) + 1
    sources = (jnp.arange(N_VERT)[:, None] + offsets) % N_VERT
    live_count = jax.random.randint(jax.random.fold_in(key, 12), (N_VERT,), 1, NB + 1)
    full_row = jax.random.randint(jax.random.fold_in(key, 13), (), 0, N_VERT)
    live_count = jnp.where(jnp.arange(N_VERT) == full_row, NB, live_count)
    return jnp.where(jnp.arange(NB)[None, :] < live_count[:, None], sources, -1).astype(jnp.int32)


def draw_halo_rows(key, part):
    keys = jax.random.split(jax.random.fold_in(key, 21), N_VERT * NB)
    picked = jax.vmap(shuffled_rows)(keys)
    return picked.reshape(N_VERT, NB, HALO).astype(jnp.int32)


def with_ends(entries, key, smallest, top_value):
    longest = entries.shape.index(max(entries.shape))
    spots = []
    for shift in (0, 1):
        where = [jax.random.randint(jax.random.fold_in(key, axis), (), 0, length) for axis, length in enumerate(entries.shape)]
        where[longest] = (where[longest] + shift) % entries.shape[longest]
        spots.append(tuple(where))
    return entries.at[spots[0]].set(smallest).at[spots[1]].set(top_value)


def shard_levels(rng, dims, cuts, smallest, largest):
    factor_of, own = 1.0, jax.random.fold_in(rng, 6)
    for position, parts in cuts:
        heights = jnp.exp(jax.random.uniform(jax.random.fold_in(own, position), (parts,), jnp.float32, smallest / len(cuts), largest / len(cuts)))
        factor_of = factor_of * jnp.repeat(heights, dims[position] // parts).reshape([-1 if axis == position else 1 for axis in range(len(dims))])
    return factor_of


def noise(own_key, dims, width, bound, cuts=(), held_as=jnp.bfloat16):
    drawn = jax.random.normal(own_key, dims, jnp.float32) * width
    if len(cuts) > 0:
        drawn = shard_levels(own_key, dims, cuts, -0.22, 0.18) * drawn
    return jnp.clip(drawn, min=-bound, max=bound).astype(held_as)


def setup_inputs(seed: int = 0) -> dict:
    splits = jax.random.split(jax.random.key(seed), 9)
    features_t = noise(splits[0], (F_IN, VERTICES), 4.0, 24.0, ((0, 4), (1, 8)))
    weight = noise(splits[1], (F_IN, F_OUT), (F_IN // 4) ** -0.5, 1.0, ((0, 4),))
    bias = noise(splits[2], (F_OUT,), 0.5, 3.0, ((0, 4),), jnp.float32)
    self_mask = with_ends((jax.random.randint(splits[3], (N_VERT, BLOCK, BLOCK), 0, BLOCK) < 16).astype(jnp.int32), jax.random.fold_in(splits[3], 1), 0, 1)
    halo_mask = with_ends((jax.random.randint(splits[4], (N_VERT, NB, BLOCK, HALO), 0, HALO) < 8).astype(jnp.int32), jax.random.fold_in(splits[4], 1), 0, 1)
    block_src = draw_block_src(jax.random.fold_in(splits[8], 71), 0)
    halo_rows = draw_halo_rows(jax.random.fold_in(splits[8], 71), 0)
    outside_degree = with_ends(jax.random.randint(splits[7], (VERTICES,), 0, 48), jax.random.fold_in(splits[7], 1), 0, 47).astype(jnp.int32)
    return dict(features_t=features_t, weight=weight, bias=bias, self_mask=self_mask, halo_mask=halo_mask, block_src=block_src, halo_rows=halo_rows, outside_degree=outside_degree)


def reference(features_t, weight, bias, self_mask, halo_mask, block_src, halo_rows, outside_degree):
    live_slot = block_src >= 0
    halo_counts = lax.optimization_barrier(jnp.sum(lax.optimization_barrier(jnp.sum(halo_mask, axis=-1)) * live_slot[:, :, None].astype(jnp.int32), axis=1))
    degree = 1 + lax.optimization_barrier(jnp.sum(self_mask, axis=-1)) + halo_counts + outside_degree.reshape(N_VERT, BLOCK)
    inverse_root = 1.0 / jnp.sqrt(degree.astype(jnp.float32))
    flat_root = inverse_root.reshape(-1)
    scaled = (features_t.astype(jnp.float32) * flat_root[None, :]).astype(jnp.bfloat16)
    scaled_wide = scaled.astype(jnp.float32)

    def one_partition(inputs):
        part_index, own_mask, slot_masks, sources, rows, root_part = inputs
        own_block = lax.dynamic_slice_in_dim(scaled_wide, (part_index * BLOCK).astype(jnp.int32), BLOCK, 1)
        summed_rows = own_block + jnp.einsum('fj,ij->fi', own_block, own_mask.astype(jnp.float32))
        column_ids = (jnp.maximum(sources, 0) * BLOCK)[:, None] + rows
        halo_vals = jnp.take(scaled_wide, column_ids.reshape(-1).astype(jnp.int32), axis=1).reshape(F_IN, NB, HALO)
        live_blocks = slot_masks.astype(jnp.float32) * (sources >= 0).astype(jnp.float32)[:, None, None]
        summed_rows = summed_rows + jnp.einsum('fsk,sik->fi', halo_vals, live_blocks)
        return (summed_rows * root_part[None, :]).astype(jnp.bfloat16)
    parts_out = lax.map(one_partition, (jnp.arange(N_VERT, dtype=jnp.int32), self_mask, halo_mask, block_src, halo_rows, inverse_root))
    aggregated = jnp.transpose(parts_out, (1, 0, 2)).reshape(F_IN, N_VERT * BLOCK)
    mixed = jnp.dot(weight.T, aggregated, preferred_element_type=jnp.float32)
    return jnp.maximum(mixed + bias[:, None], 0.0).astype(jnp.bfloat16)
```

```python
import functools

import jax
import jax.numpy as jnp
from jax import lax
from jax.experimental import pallas as pl
from jax.experimental.pallas import tpu as pltpu
from jax.sharding import PartitionSpec as P

MESH = pl.DeviceIdType.MESH
LANES = 128
NT = (((1,), (1,)), ((), ()))
NN = (((1,), (0,)), ((), ()))


def lane_gather(table, index):
    parts = []
    for start in range(0, index.shape[1], LANES):
        wanted = index[:, start : start + LANES]
        low, high = wanted % LANES, wanted // LANES
        picked = jnp.zeros(wanted.shape, table.dtype)
        for piece in range(table.shape[1] // LANES):
            seen = jnp.take_along_axis(
                table[:, piece * LANES : (piece + 1) * LANES], low, axis=1, mode="promise_in_bounds"
            )
            picked = jnp.where(high == piece, seen, picked)
        parts.append(picked)
    return jnp.concatenate(parts, axis=1)


def kernel(
    n_vert, n_af, n_chunk,
    feat, weight, bias, self_mask, halo_mask, sources, rows, outside,
    out,
    feat_all, weight_all, bias_v, self_v, halo_v, source_s, rows_v, outside_v,
    root_all, agg_all, self_b, halo_b, weight_t, root_pick,
    small_sem, self_sem, halo_sem,
    feat_send, feat_recv, weight_send, weight_recv, root_send, root_recv, agg_send, agg_recv,
):
    my_vert, my_af = lax.axis_index("vert"), lax.axis_index("af")
    n_slot, block, halo = halo_v.shape
    span = block // n_chunk

    small = [
        pltpu.make_async_copy(src, dst, small_sem.at[i])
        for i, (src, dst) in enumerate((
            (sources, source_s),
            (outside, outside_v),
            (feat, feat_all.at[my_vert]),
            (rows, rows_v),
            (weight, weight_all.at[my_af]),
            (bias, bias_v),
        ))
    ]
    own_copies, halo_copies = [], []
    small[0].start()
    for c in range(n_chunk):
        part = pl.ds(c * span, span)
        halo_copies.append(
            pltpu.make_async_copy(halo_mask.at[:, part, :], halo_v.at[:, part, :], halo_sem.at[c])
        )
        own_copies.append(pltpu.make_async_copy(self_mask.at[part, :], self_v.at[part, :], self_sem.at[c]))
        halo_copies[c].start()
        own_copies[c].start()
    for copy in small[1:]:
        copy.start()

    barrier = pltpu.get_barrier_semaphore()
    for k in range(1, n_vert):
        pl.semaphore_signal(barrier, inc=1, device_id={"vert": lax.rem(my_vert + k, n_vert)}, device_id_type=MESH)
    for k in range(1, n_af):
        pl.semaphore_signal(barrier, inc=1, device_id={"af": lax.rem(my_af + k, n_af)}, device_id_type=MESH)
    pl.semaphore_wait(barrier, n_vert + n_af - 2)

    def to_vert(src, dst, send, recv):
        copies = [
            pltpu.make_async_remote_copy(
                src_ref=src, dst_ref=dst, send_sem=send.at[k], recv_sem=recv.at[k],
                device_id={"vert": lax.rem(my_vert + k, n_vert)}, device_id_type=MESH,
            )
            for k in range(1, n_vert)
        ]
        for copy in copies:
            copy.start()
        return copies

    def to_af(src, dst, send, recv):
        copies = [
            pltpu.make_async_remote_copy(
                src_ref=src, dst_ref=dst, send_sem=send.at[k], recv_sem=recv.at[k],
                device_id={"af": lax.rem(my_af + k, n_af)}, device_id_type=MESH,
            )
            for k in range(1, n_af)
        ]
        for copy in copies:
            copy.start()
        return copies

    feat_copies = to_vert(feat, feat_all.at[my_vert], feat_send, feat_recv)
    weight_copies = to_af(weight, weight_all.at[my_af], weight_send, weight_recv)

    small[0].wait()
    small[1].wait()
    source = [source_s[0, s] for s in range(n_slot)]
    live = [jnp.where(src >= 0, 1.0, 0.0).astype(jnp.float32) for src in source]
    source = [jnp.maximum(src, 0) for src in source]
    ones = jnp.ones((8, halo), jnp.bfloat16)
    for c in range(n_chunk):
        part = pl.ds(c * span, span)
        halo_copies[c].wait()
        own_copies[c].wait()
        count = jnp.zeros((span, halo), jnp.bfloat16)
        for j in range(0, block, halo):
            entries = self_v[part, j : j + halo].astype(jnp.float32).astype(jnp.bfloat16)
            self_b[part, j : j + halo] = entries
            count = count + entries
        for s in range(n_slot):
            entries = (halo_v[s, part, :].astype(jnp.float32) * live[s]).astype(jnp.bfloat16)
            halo_b[part, s * halo : (s + 1) * halo] = entries
            count = count + entries
        edges = lax.dot_general(ones, count, NT, preferred_element_type=jnp.float32)[0:1]
        degree = 1.0 + edges + outside_v[:, part].astype(jnp.float32)
        root_all[my_vert, :, part] = 1.0 / jnp.sqrt(degree)
    root_copies = to_vert(root_all.at[my_vert], root_all.at[my_vert], root_send, root_recv)

    root = root_all[my_vert]
    small[2].wait()
    scaled = (feat_all[my_vert].astype(jnp.float32) * root).astype(jnp.bfloat16)
    summed = scaled.astype(jnp.float32) + lax.dot_general(scaled, self_b[...], NT, preferred_element_type=jnp.float32)

    small[3].wait()
    index = jnp.concatenate([rows_v[...], jnp.zeros((8 - n_slot, halo), jnp.int32)], axis=0)
    for copy in feat_copies:
        copy.wait_recv()
    column = lax.broadcasted_iota(jnp.int32, (block, halo), 0)
    picked = []
    for s in range(n_slot):
        chosen = (column == rows_v[s : s + 1, :]).astype(jnp.float32).astype(jnp.bfloat16)
        picked.append(
            lax.dot_general(feat_all[source[s]], chosen, NN, preferred_element_type=jnp.float32)
        )

    small[4].wait()
    small[5].wait()
    for copy in weight_copies:
        copy.wait_recv()
    f_in = weight_all.shape[0] * weight_all.shape[1]
    whole = weight_all[...].astype(jnp.float32).reshape(f_in, weight_all.shape[2])
    weight_t[...] = whole.T.astype(jnp.bfloat16)
    out_rows = out.shape[0]
    weight_cols = weight_t[pl.ds(pl.multiple_of(my_af * out_rows, out_rows), out_rows), :]
    square = (out_rows, out_rows)
    diagonal = lax.broadcasted_iota(jnp.int32, square, 0) == lax.broadcasted_iota(jnp.int32, square, 1)
    offset = jnp.sum(jnp.where(diagonal, jnp.broadcast_to(bias_v[...], square), 0.0), axis=1, keepdims=True)

    for copy in root_copies:
        copy.wait_recv()
    root_pick[...] = jnp.zeros_like(root_pick)
    for s in range(n_slot):
        root_pick[s : s + 1, :] = root_all[source[s]]
    roots = lane_gather(root_pick[...], index)
    values = jnp.concatenate(
        [(picked[s] * roots[s : s + 1, :]).astype(jnp.bfloat16) for s in range(n_slot)], axis=1
    )
    summed = summed + lax.dot_general(values, halo_b[...], NT, preferred_element_type=jnp.float32)
    agg_all[my_af] = (summed * root).astype(jnp.bfloat16)
    agg_copies = to_af(agg_all.at[my_af], agg_all.at[my_af], agg_send, agg_recv)
    for copy in feat_copies + weight_copies + root_copies:
        copy.wait_send()
    for copy in agg_copies:
        copy.wait_recv()
    mixed = lax.dot_general(
        weight_cols, agg_all[...].reshape(f_in, block), NN, preferred_element_type=jnp.float32
    )
    out[...] = jnp.maximum(mixed + offset, 0.0).astype(jnp.bfloat16)
    for copy in agg_copies:
        copy.wait_send()


def solution(mesh):
    n_vert, n_af = mesh.shape["vert"], mesh.shape["af"]

    def body(features_t, weight, bias, self_mask, halo_mask, block_src, halo_rows, outside_degree):
        feat_count, block = features_t.shape
        n_slot, halo = halo_rows.shape[1:]
        out_rows = bias.shape[0]
        n_chunk = 4
        anywhere = pl.BlockSpec(memory_space=pl.ANY)
        return pl.pallas_call(
            functools.partial(kernel, n_vert, n_af, n_chunk),
            out_shape=jax.ShapeDtypeStruct((out_rows, block), jnp.bfloat16),
            in_specs=[anywhere] * 8,
            out_specs=pl.BlockSpec(memory_space=pltpu.VMEM),
            scratch_shapes=[
                pltpu.VMEM((n_vert, feat_count, block), jnp.bfloat16),
                pltpu.VMEM((n_af,) + weight.shape, jnp.bfloat16),
                pltpu.VMEM((1, out_rows), jnp.float32),
                pltpu.VMEM((block, block), jnp.int32),
                pltpu.VMEM((n_slot, block, halo), jnp.int32),
                pltpu.SMEM((1, n_slot), jnp.int32),
                pltpu.VMEM((n_slot, halo), jnp.int32),
                pltpu.VMEM((1, block), jnp.int32),
                pltpu.VMEM((n_vert, 1, block), jnp.float32),
                pltpu.VMEM((n_af, feat_count, block), jnp.bfloat16),
                pltpu.VMEM((block, block), jnp.bfloat16),
                pltpu.VMEM((block, n_slot * halo), jnp.bfloat16),
                pltpu.VMEM((weight.shape[1], n_af * feat_count), jnp.bfloat16),
                pltpu.VMEM((8, block), jnp.float32),
                pltpu.SemaphoreType.DMA((6,)),
                pltpu.SemaphoreType.DMA((n_chunk,)),
                pltpu.SemaphoreType.DMA((n_chunk,)),
                pltpu.SemaphoreType.DMA((n_vert,)),
                pltpu.SemaphoreType.DMA((n_vert,)),
                pltpu.SemaphoreType.DMA((n_af,)),
                pltpu.SemaphoreType.DMA((n_af,)),
                pltpu.SemaphoreType.DMA((n_vert,)),
                pltpu.SemaphoreType.DMA((n_vert,)),
                pltpu.SemaphoreType.DMA((n_af,)),
                pltpu.SemaphoreType.DMA((n_af,)),
            ],
            compiler_params=pltpu.CompilerParams(collective_id=0, has_side_effects=True),
        )(
            features_t, weight, bias.reshape(1, -1), self_mask[0], halo_mask[0], block_src,
            halo_rows[0], outside_degree.reshape(1, -1),
        )

    return jax.shard_map(
        body,
        mesh=mesh,
        in_specs=(
            P("af", "vert"),
            P("af", None),
            P("af"),
            P("vert", None, None),
            P("vert", None, None, None),
            P("vert", None),
            P("vert", None, None),
            P("vert"),
        ),
        out_specs=P("af", "vert"),
        check_vma=False,
    )
```

```python
import functools

import jax
import jax.numpy as jnp
from jax import lax
from jax.experimental import pallas as pl
from jax.experimental.pallas import tpu as pltpu
from jax.sharding import PartitionSpec as P

MESH = pl.DeviceIdType.MESH
LANES = 128
NT = (((1,), (1,)), ((), ()))
NN = (((1,), (0,)), ((), ()))


def lane_gather(table, index):
    parts = []
    for start in range(0, index.shape[1], LANES):
        wanted = index[:, start : start + LANES]
        low, high = wanted % LANES, wanted // LANES
        picked = jnp.zeros(wanted.shape, table.dtype)
        for piece in range(table.shape[1] // LANES):
            seen = jnp.take_along_axis(
                table[:, piece * LANES : (piece + 1) * LANES], low, axis=1, mode="promise_in_bounds"
            )
            picked = jnp.where(high == piece, seen, picked)
        parts.append(picked)
    return jnp.concatenate(parts, axis=1)


def kernel(
    n_vert, n_af, n_chunk,
    feat, weight, bias, self_mask, halo_mask, sources, rows, outside,
    out,
    feat_all, weight_all, bias_v, self_v, halo_v, source_s, rows_v, outside_v,
    root_all, agg_all, self_b, halo_b, weight_t, root_pick, row_pick,
    small_sem, self_sem, halo_sem,
    feat_send, feat_recv, weight_send, weight_recv, root_send, root_recv, agg_send, agg_recv,
):
    my_vert, my_af = lax.axis_index("vert"), lax.axis_index("af")
    n_slot, block, halo = halo_v.shape
    span = block // n_chunk

    small = [
        pltpu.make_async_copy(src, dst, small_sem.at[i])
        for i, (src, dst) in enumerate((
            (sources, source_s),
            (outside, outside_v),
            (feat, feat_all.at[my_vert]),
            (rows, rows_v),
            (weight, weight_all.at[my_af]),
            (bias, bias_v),
        ))
    ]
    own_copies, halo_copies = [], []
    small[2].start()
    small[0].start()
    for c in range(n_chunk):
        part = pl.ds(c * span, span)
        halo_copies.append(
            pltpu.make_async_copy(halo_mask.at[:, part, :], halo_v.at[:, part, :], halo_sem.at[c])
        )
        own_copies.append(pltpu.make_async_copy(self_mask.at[part, :], self_v.at[part, :], self_sem.at[c]))
        halo_copies[c].start()
        own_copies[c].start()
    for i in (1, 3, 4, 5):
        small[i].start()

    barrier = pltpu.get_barrier_semaphore()
    for k in range(1, n_vert):
        pl.semaphore_signal(barrier, inc=1, device_id={"vert": lax.rem(my_vert + k, n_vert)}, device_id_type=MESH)
    for k in range(1, n_af):
        pl.semaphore_signal(barrier, inc=1, device_id={"af": lax.rem(my_af + k, n_af)}, device_id_type=MESH)
    pl.semaphore_wait(barrier, n_vert + n_af - 2)

    def to_vert(src, dst, send, recv):
        copies = [
            pltpu.make_async_remote_copy(
                src_ref=src, dst_ref=dst, send_sem=send.at[k], recv_sem=recv.at[k],
                device_id={"vert": lax.rem(my_vert + k, n_vert)}, device_id_type=MESH,
            )
            for k in range(1, n_vert)
        ]
        for copy in copies:
            copy.start()
        return copies

    def to_af(src, dst, send, recv):
        copies = [
            pltpu.make_async_remote_copy(
                src_ref=src, dst_ref=dst, send_sem=send.at[k], recv_sem=recv.at[k],
                device_id={"af": lax.rem(my_af + k, n_af)}, device_id_type=MESH,
            )
            for k in range(1, n_af)
        ]
        for copy in copies:
            copy.start()
        return copies

    small[2].wait()
    feat_copies = to_vert(feat_all.at[my_vert], feat_all.at[my_vert], feat_send, feat_recv)
    weight_copies = to_af(weight, weight_all.at[my_af], weight_send, weight_recv)

    small[0].wait()
    small[1].wait()
    source = [source_s[0, s] for s in range(n_slot)]
    live = [jnp.where(src >= 0, 1.0, 0.0).astype(jnp.float32) for src in source]
    source = [jnp.maximum(src, 0) for src in source]
    ones = jnp.ones((8, halo), jnp.bfloat16)
    for c in range(n_chunk):
        part = pl.ds(c * span, span)
        halo_copies[c].wait()
        own_copies[c].wait()
        count = jnp.zeros((span, halo), jnp.bfloat16)
        for j in range(0, block, halo):
            entries = self_v[part, j : j + halo].astype(jnp.float32).astype(jnp.bfloat16)
            self_b[part, j : j + halo] = entries
            count = count + entries
        for s in range(n_slot):
            entries = (halo_v[s, part, :].astype(jnp.float32) * live[s]).astype(jnp.bfloat16)
            halo_b[part, s * halo : (s + 1) * halo] = entries
            count = count + entries
        edges = lax.dot_general(ones, count, NT, preferred_element_type=jnp.float32)[0:1]
        degree = 1.0 + edges + outside_v[:, part].astype(jnp.float32)
        root_all[my_vert, :, part] = 1.0 / jnp.sqrt(degree)
    root_copies = to_vert(root_all.at[my_vert], root_all.at[my_vert], root_send, root_recv)

    root = root_all[my_vert]
    scaled = (feat_all[my_vert].astype(jnp.float32) * root).astype(jnp.bfloat16)
    summed = scaled.astype(jnp.float32) + lax.dot_general(scaled, self_b[...], NT, preferred_element_type=jnp.float32)

    small[3].wait()
    row_pick[...] = jnp.zeros_like(row_pick)
    for s in range(n_slot):
        row_pick[s : s + 1, :] = rows_v[s]
    index = row_pick[...]
    for copy in feat_copies:
        copy.wait_recv()
    column = lax.broadcasted_iota(jnp.int32, (block, halo), 0)
    picked = []
    for s in range(n_slot):
        chosen = (column == rows_v[s]).astype(jnp.float32).astype(jnp.bfloat16)
        picked.append(
            lax.dot_general(feat_all[source[s]], chosen, NN, preferred_element_type=jnp.float32)
        )

    small[4].wait()
    small[5].wait()
    for copy in weight_copies:
        copy.wait_recv()
    f_in = weight_all.shape[0] * weight_all.shape[1]
    whole = weight_all[...].astype(jnp.float32).reshape(f_in, weight_all.shape[2])
    weight_t[...] = whole.T.astype(jnp.bfloat16)
    out_rows = out.shape[0]
    weight_cols = weight_t[pl.ds(pl.multiple_of(my_af * out_rows, out_rows), out_rows), :]
    square = (out_rows, out_rows)
    diagonal = lax.broadcasted_iota(jnp.int32, square, 0) == lax.broadcasted_iota(jnp.int32, square, 1)
    offset = jnp.sum(jnp.where(diagonal, jnp.broadcast_to(bias_v[...], square), 0.0), axis=1, keepdims=True)

    for copy in root_copies:
        copy.wait_recv()
    root_pick[...] = jnp.zeros_like(root_pick)
    for s in range(n_slot):
        root_pick[s : s + 1, :] = root_all[source[s]]
    roots = lane_gather(root_pick[...], index)
    values = jnp.concatenate(
        [(picked[s] * roots[s : s + 1, :]).astype(jnp.bfloat16) for s in range(n_slot)], axis=1
    )
    halves = []
    for h in range(2):
        part = pl.ds(h * (block // 2), block // 2)
        total = summed[:, h * (block // 2) : (h + 1) * (block // 2)] + lax.dot_general(
            values, halo_b[part, :], NT, preferred_element_type=jnp.float32
        )
        agg_all[my_af, :, part] = (total * root_all[my_vert, :, part]).astype(jnp.bfloat16)
        sent = agg_all.at[my_af, :, part]
        halves.append(to_af(sent, sent, agg_send.at[h], agg_recv.at[h]))
    for copy in feat_copies + weight_copies + root_copies:
        copy.wait_send()
    for h in range(2):
        part = pl.ds(h * (block // 2), block // 2)
        for copy in halves[h]:
            copy.wait_recv()
        mixed = lax.dot_general(
            weight_cols, agg_all[:, :, part].reshape(f_in, block // 2), NN, preferred_element_type=jnp.float32
        )
        out[:, part] = (mixed + offset).astype(jnp.bfloat16)
    for copy in halves[0] + halves[1]:
        copy.wait_send()


def solution(mesh):
    n_vert, n_af = mesh.shape["vert"], mesh.shape["af"]

    def body(features_t, weight, bias, self_mask, halo_mask, block_src, halo_rows, outside_degree):
        feat_count, block = features_t.shape
        n_slot, halo = halo_rows.shape[1:]
        out_rows = bias.shape[0]
        n_chunk = 4
        anywhere = pl.BlockSpec(memory_space=pltpu.HBM)
        mixed = pl.pallas_call(
            functools.partial(kernel, n_vert, n_af, n_chunk),
            out_shape=jax.ShapeDtypeStruct((out_rows, block), jnp.bfloat16),
            in_specs=[anywhere] * 8,
            out_specs=pl.BlockSpec(memory_space=pltpu.VMEM),
            scratch_shapes=[
                pltpu.VMEM((n_vert, feat_count, block), jnp.bfloat16),
                pltpu.VMEM((n_af,) + weight.shape, jnp.bfloat16),
                pltpu.VMEM((1, out_rows), jnp.float32),
                pltpu.VMEM((block, block), jnp.int32),
                pltpu.VMEM((n_slot, block, halo), jnp.int32),
                pltpu.SMEM((1, n_slot), jnp.int32),
                pltpu.VMEM((n_slot, 1, halo), jnp.int32),
                pltpu.VMEM((1, block), jnp.int32),
                pltpu.VMEM((n_vert, 1, block), jnp.float32),
                pltpu.VMEM((n_af, feat_count, block), jnp.bfloat16),
                pltpu.VMEM((block, block), jnp.bfloat16),
                pltpu.VMEM((block, n_slot * halo), jnp.bfloat16),
                pltpu.VMEM((weight.shape[1], n_af * feat_count), jnp.bfloat16),
                pltpu.VMEM((8, block), jnp.float32),
                pltpu.VMEM((8, halo), jnp.int32),
                pltpu.SemaphoreType.DMA((6,)),
                pltpu.SemaphoreType.DMA((n_chunk,)),
                pltpu.SemaphoreType.DMA((n_chunk,)),
                pltpu.SemaphoreType.DMA((n_vert,)),
                pltpu.SemaphoreType.DMA((n_vert,)),
                pltpu.SemaphoreType.DMA((n_af,)),
                pltpu.SemaphoreType.DMA((n_af,)),
                pltpu.SemaphoreType.DMA((n_vert,)),
                pltpu.SemaphoreType.DMA((n_vert,)),
                pltpu.SemaphoreType.DMA((2, n_af)),
                pltpu.SemaphoreType.DMA((2, n_af)),
            ],
            compiler_params=pltpu.CompilerParams(
                collective_id=0, has_side_effects=True, vmem_limit_bytes=24 * 1024 * 1024
            ),
        )(*(
            pltpu.with_memory_space_constraint(each, pltpu.HBM)
            for each in (
                features_t, weight, bias.reshape(1, -1), self_mask[0], halo_mask[0], block_src,
                jnp.swapaxes(halo_rows, 0, 1), outside_degree.reshape(1, -1),
            )
        ))
        return jnp.maximum(mixed, 0)

    return jax.shard_map(
        body,
        mesh=mesh,
        in_specs=(
            P("af", "vert"),
            P("af", None),
            P("af"),
            P("vert", None, None),
            P("vert", None, None, None),
            P("vert", None),
            P("vert", None, None),
            P("vert"),
        ),
        out_specs=P("af", "vert"),
        check_vma=False,
    )
```

```python
import functools

import jax
import jax.numpy as jnp
from jax import lax
from jax.experimental import pallas as pl
from jax.experimental.pallas import tpu as pltpu
from jax.sharding import PartitionSpec as P

MESH = pl.DeviceIdType.MESH
LANES = 128
NT = (((1,), (1,)), ((), ()))
NN = (((1,), (0,)), ((), ()))


def lane_gather(table, index):
    parts = []
    for start in range(0, index.shape[1], LANES):
        wanted = index[:, start : start + LANES]
        low, high = wanted % LANES, wanted // LANES
        picked = jnp.zeros(wanted.shape, table.dtype)
        for piece in range(table.shape[1] // LANES):
            seen = jnp.take_along_axis(
                table[:, piece * LANES : (piece + 1) * LANES], low, axis=1, mode="promise_in_bounds"
            )
            picked = jnp.where(high == piece, seen, picked)
        parts.append(picked)
    return jnp.concatenate(parts, axis=1)


def kernel(
    n_vert, n_af, n_chunk,
    feat, weight, bias, self_mask, halo_mask, sources, rows, outside,
    out,
    feat_all, weight_all, bias_v, self_v, halo_v, source_s, rows_v, outside_v,
    root_all, agg_all, self_b, halo_b, weight_t, root_pick, row_pick, chosen, halo_t,
    small_sem, self_sem, halo_sem,
    feat_send, feat_recv, weight_send, weight_recv, root_send, root_recv, agg_send, agg_recv,
):
    my_vert, my_af = lax.axis_index("vert"), lax.axis_index("af")
    n_slot, block, halo = halo_v.shape
    span = block // n_chunk

    barrier = pltpu.get_barrier_semaphore()
    for k in range(1, n_vert):
        pl.semaphore_signal(barrier, inc=1, device_id={"vert": lax.rem(my_vert + k, n_vert)}, device_id_type=MESH)
    for k in range(1, n_af):
        pl.semaphore_signal(barrier, inc=1, device_id={"af": lax.rem(my_af + k, n_af)}, device_id_type=MESH)

    small = [
        pltpu.make_async_copy(src, dst, small_sem.at[i])
        for i, (src, dst) in enumerate((
            (sources, source_s),
            (outside, outside_v),
            (feat, feat_all.at[my_vert]),
            (rows, rows_v),
            (weight, weight_all.at[my_af]),
            (bias, bias_v),
        ))
    ]
    own_copies, halo_copies = [], []
    small[2].start()
    small[0].start()
    for c in range(n_chunk):
        part = pl.ds(c * span, span)
        halo_copies.append(
            pltpu.make_async_copy(halo_mask.at[:, part, :], halo_v.at[:, part, :], halo_sem.at[c])
        )
        own_copies.append(pltpu.make_async_copy(self_mask.at[part, :], self_v.at[part, :], self_sem.at[c]))
        halo_copies[c].start()
        own_copies[c].start()
    for i in (1, 3, 4, 5):
        small[i].start()

    pl.semaphore_wait(barrier, n_vert + n_af - 2)

    def to_vert(src, dst, send, recv):
        copies = [
            pltpu.make_async_remote_copy(
                src_ref=src, dst_ref=dst, send_sem=send.at[k], recv_sem=recv.at[k],
                device_id={"vert": lax.rem(my_vert + k, n_vert)}, device_id_type=MESH,
            )
            for k in range(1, n_vert)
        ]
        for copy in copies:
            copy.start()
        return copies

    def to_af(src, dst, send, recv):
        copies = [
            pltpu.make_async_remote_copy(
                src_ref=src, dst_ref=dst, send_sem=send.at[k], recv_sem=recv.at[k],
                device_id={"af": lax.rem(my_af + k, n_af)}, device_id_type=MESH,
            )
            for k in range(1, n_af)
        ]
        for copy in copies:
            copy.start()
        return copies

    small[2].wait()
    group = n_vert // 2 if n_vert % 2 == 0 else n_vert
    n_step = 2 if group < n_vert else 0
    depth = feat.shape[0] // max(n_step, 1)
    base, place = my_vert // group * group, lax.rem(my_vert, group)
    partner = lax.rem(my_vert + group, n_vert)

    def feature_copy(ref, i, target):
        return pltpu.make_async_remote_copy(
            src_ref=ref, dst_ref=ref, send_sem=feat_send.at[i], recv_sem=feat_recv.at[i],
            device_id={"vert": target}, device_id_type=MESH,
        )

    def near(j):
        return base + lax.rem(place + j, group)

    across = [
        feature_copy(feat_all.at[my_vert, pl.ds(h * depth, depth), :], h, partner) for h in range(n_step)
    ]
    feat_copies = across + [
        feature_copy(feat_all.at[my_vert], n_step + j, near(j)) for j in range(1, group)
    ]
    for copy in feat_copies:
        copy.start()
    weight_copies = to_af(weight, weight_all.at[my_af], weight_send, weight_recv)

    small[0].wait()
    small[1].wait()
    source = [source_s[0, s] for s in range(n_slot)]
    live = [jnp.where(src >= 0, 1.0, 0.0).astype(jnp.float32) for src in source]
    source = [jnp.maximum(src, 0) for src in source]
    ones = jnp.ones((8, halo), jnp.bfloat16)
    for c in range(n_chunk):
        part = pl.ds(c * span, span)
        halo_copies[c].wait()
        own_copies[c].wait()
        count = jnp.zeros((span, halo), jnp.bfloat16)
        for j in range(0, block, halo):
            entries = self_v[part, j : j + halo].astype(jnp.float32).astype(jnp.bfloat16)
            self_b[part, j : j + halo] = entries
            count = count + entries
        for s in range(n_slot):
            entries = (halo_v[s, part, :].astype(jnp.float32) * live[s]).astype(jnp.bfloat16)
            halo_b[part, s * halo : (s + 1) * halo] = entries
            count = count + entries
        edges = lax.dot_general(ones, count, NT, preferred_element_type=jnp.float32)[0:1]
        degree = 1.0 + edges + outside_v[:, part].astype(jnp.float32)
        root_all[my_vert, :, part] = 1.0 / jnp.sqrt(degree)
    root_copies = to_vert(root_all.at[my_vert], root_all.at[my_vert], root_send, root_recv)

    for h in range(n_step):
        across[h].wait_recv()
        for j in range(1, group):
            passed = feature_copy(
                feat_all.at[partner, pl.ds(h * depth, depth), :], n_step + (h + 1) * group + j, near(j)
            )
            passed.start()
            feat_copies.append(passed)

    root = root_all[my_vert]
    scaled = (feat_all[my_vert].astype(jnp.float32) * root).astype(jnp.bfloat16)
    summed = scaled.astype(jnp.float32) + lax.dot_general(scaled, self_b[...], NT, preferred_element_type=jnp.float32)

    small[3].wait()
    row_pick[...] = jnp.zeros_like(row_pick)
    for s in range(n_slot):
        row_pick[s : s + 1, :] = rows_v[s]
    index = row_pick[...]
    column = lax.broadcasted_iota(jnp.int32, (block, halo), 0)
    for s in range(n_slot):
        chosen[s] = (column == rows_v[s]).astype(jnp.float32).astype(jnp.bfloat16)

    small[4].wait()
    small[5].wait()
    for copy in weight_copies:
        copy.wait_recv()
    f_in = weight_all.shape[0] * weight_all.shape[1]
    whole = weight_all[...].astype(jnp.float32).reshape(f_in, weight_all.shape[2])
    weight_t[...] = whole.T.astype(jnp.bfloat16)
    out_rows = out.shape[0]
    weight_cols = weight_t[pl.ds(pl.multiple_of(my_af * out_rows, out_rows), out_rows), :]
    square = (out_rows, out_rows)
    diagonal = lax.broadcasted_iota(jnp.int32, square, 0) == lax.broadcasted_iota(jnp.int32, square, 1)
    offset = jnp.sum(jnp.where(diagonal, jnp.broadcast_to(bias_v[...], square), 0.0), axis=1, keepdims=True)

    halo_t[...] = halo_b[...].T
    for copy in feat_copies[n_step:]:
        copy.wait_recv()
    picked = [
        lax.dot_general(feat_all[source[s]], chosen[s], NN, preferred_element_type=jnp.float32)
        for s in range(n_slot)
    ]

    for copy in root_copies:
        copy.wait_recv()
    root_pick[...] = jnp.zeros_like(root_pick)
    for s in range(n_slot):
        root_pick[s : s + 1, :] = root_all[source[s]]
    roots = lane_gather(root_pick[...], index)
    values = jnp.concatenate(
        [(picked[s] * roots[s : s + 1, :]).astype(jnp.bfloat16) for s in range(n_slot)], axis=1
    )
    halves = []
    for h in range(2):
        part = pl.ds(h * (block // 2), block // 2)
        total = summed[:, h * (block // 2) : (h + 1) * (block // 2)] + lax.dot_general(
            values, halo_t[:, part], NN, preferred_element_type=jnp.float32
        )
        agg_all[my_af, :, part] = (total * root_all[my_vert, :, part]).astype(jnp.bfloat16)
        sent = agg_all.at[my_af, :, part]
        halves.append(to_af(sent, sent, agg_send.at[h], agg_recv.at[h]))
    for copy in feat_copies + weight_copies + root_copies:
        copy.wait_send()
    for h in range(2):
        part = pl.ds(h * (block // 2), block // 2)
        for copy in halves[h]:
            copy.wait_recv()
        mixed = lax.dot_general(
            weight_cols, agg_all[:, :, part].reshape(f_in, block // 2), NN, preferred_element_type=jnp.float32
        )
        out[:, part] = (mixed + offset).astype(jnp.bfloat16)
    for copy in halves[0] + halves[1]:
        copy.wait_send()


def solution(mesh):
    n_vert, n_af = mesh.shape["vert"], mesh.shape["af"]

    def body(features_t, weight, bias, self_mask, halo_mask, block_src, halo_rows, outside_degree):
        feat_count, block = features_t.shape
        n_slot, halo = halo_rows.shape[1:]
        out_rows = bias.shape[0]
        n_chunk = 4
        anywhere = pl.BlockSpec(memory_space=pltpu.HBM)
        mixed = pl.pallas_call(
            functools.partial(kernel, n_vert, n_af, n_chunk),
            out_shape=jax.ShapeDtypeStruct((out_rows, block), jnp.bfloat16),
            in_specs=[anywhere] * 8,
            out_specs=pl.BlockSpec(memory_space=pltpu.VMEM),
            scratch_shapes=[
                pltpu.VMEM((n_vert, feat_count, block), jnp.bfloat16),
                pltpu.VMEM((n_af,) + weight.shape, jnp.bfloat16),
                pltpu.VMEM((1, out_rows), jnp.float32),
                pltpu.VMEM((block, block), jnp.int32),
                pltpu.VMEM((n_slot, block, halo), jnp.int32),
                pltpu.SMEM((1, n_slot), jnp.int32),
                pltpu.VMEM((n_slot, 1, halo), jnp.int32),
                pltpu.VMEM((1, block), jnp.int32),
                pltpu.VMEM((n_vert, 1, block), jnp.float32),
                pltpu.VMEM((n_af, feat_count, block), jnp.bfloat16),
                pltpu.VMEM((block, block), jnp.bfloat16),
                pltpu.VMEM((block, n_slot * halo), jnp.bfloat16),
                pltpu.VMEM((weight.shape[1], n_af * feat_count), jnp.bfloat16),
                pltpu.VMEM((8, block), jnp.float32),
                pltpu.VMEM((8, halo), jnp.int32),
                pltpu.VMEM((n_slot, block, halo), jnp.bfloat16),
                pltpu.VMEM((n_slot * halo, block), jnp.bfloat16),
                pltpu.SemaphoreType.DMA((6,)),
                pltpu.SemaphoreType.DMA((n_chunk,)),
                pltpu.SemaphoreType.DMA((n_chunk,)),
                pltpu.SemaphoreType.DMA((2 * n_vert + 2,)),
                pltpu.SemaphoreType.DMA((2 * n_vert + 2,)),
                pltpu.SemaphoreType.DMA((n_af,)),
                pltpu.SemaphoreType.DMA((n_af,)),
                pltpu.SemaphoreType.DMA((n_vert,)),
                pltpu.SemaphoreType.DMA((n_vert,)),
                pltpu.SemaphoreType.DMA((2, n_af)),
                pltpu.SemaphoreType.DMA((2, n_af)),
            ],
            compiler_params=pltpu.CompilerParams(
                collective_id=0, has_side_effects=True, vmem_limit_bytes=24 * 1024 * 1024
            ),
        )(*(
            pltpu.with_memory_space_constraint(each, pltpu.HBM)
            for each in (
                features_t, weight, bias.reshape(1, -1), self_mask[0], halo_mask[0], block_src,
                jnp.swapaxes(halo_rows, 0, 1), outside_degree.reshape(1, -1),
            )
        ))
        return jnp.maximum(mixed, 0)

    return jax.shard_map(
        body,
        mesh=mesh,
        in_specs=(
            P("af", "vert"),
            P("af", None),
            P("af"),
            P("vert", None, None),
            P("vert", None, None, None),
            P("vert", None),
            P("vert", None, None),
            P("vert"),
        ),
        out_specs=P("af", "vert"),
        check_vma=False,
    )
```
